128 devices in a mesh: trial: 16 (over y, x_hi, core), feat: 8 (over x_lo, z).
Axes of the slice: x: 4 (x_hi: 2, x_lo: 2; x = x_hi * 2 + x_lo), y: 4, z: 4, core: 2. Of those that a mesh axis runs over, the one named last changes fastest.
Arguments:
- data: bfloat16 [32768, 256, 128], P('trial', 'feat'), may hold values from -2000 to 2000
- rotations: bfloat16 [768, 32768], P('feat', 'trial'), may hold values from -0.046875 to 0.046875
- span_order: int32 [6], replicated, may hold values from 0 to 5, each once
- adjacency: int32 [128, 128], replicated, may hold values from 0 to 1, as said below
- kernel: float32 [9], replicated, may hold values from 0.1 to 1
Outputs:
- enhanced: float32 [768, 256, 128], P('trial', 'feat')
The draws below stay inside these ranges and needn't reach their ends.
Inputs may be any that keep to these rules, and one draw needn't show every extreme that they name: `adjacency`: symmetric 0/1 matrix with zero diagonal.
All inputs are finite; a program needn't handle non-finite values.
Results may differ from the reference program's by a relative error of at most 0.0003.
Values may be sent and summed in bfloat16 or wider, within the bound.
A program may use at most 128 MiB of HBM per device.

```python
import math
import jax
import jax.numpy as jnp
from jax import lax

SENS = 128
ROT = 768
SPAN = 128
KERN = 9
SPANS = 6
TIMES = 256
TRIALS = 32768


def draw_data(key, part):
    keys = jax.random.split(jax.random.fold_in(key, 11), 3)
    place = jnp.arange(TRIALS, dtype=jnp.float32) / TRIALS
    rising = 10.0 ** place
    trial_scale = rising * jnp.exp(jax.random.uniform(keys[0], (TRIALS,), jnp.float32, -0.35, 0.35))
    feature_scale = 10.0 ** jax.random.uniform(keys[1], (TIMES, SENS), jnp.float32, 0.0, 1.0)
    noise = jnp.clip(jax.random.normal(keys[2], (TRIALS, TIMES, SENS), jnp.float32), -4.0, 4.0)
    values = noise * trial_scale[:, None, None] * feature_scale[None, :, :]
    return values.astype(jnp.bfloat16)


def draw_adjacency(key, part):
    picks = jax.random.randint(jax.random.fold_in(key, 23), (SENS, SENS), 0, 10)
    linked = jnp.where(picks < 1, 1, 0).astype(jnp.int32)
    linked = jnp.maximum(linked, linked.T)
    return (linked * (1 - jnp.eye(SENS, dtype=jnp.int32))).astype(jnp.int32)


def with_spikes(entries, key, source, target, parts, factor):
    def block_of(position):
        return (jnp.arange(entries.shape[position]) // (entries.shape[position] // parts)).reshape((-1,) + (1,) * (entries.ndim - 1 - position))

    near = jax.random.permutation(key, parts)[block_of(target)]
    other_side = (block_of(target) + parts // 2) % parts
    return jnp.where((block_of(source) == near) | (block_of(source) == other_side), factor * entries, entries)


def level_of(own_key, extent, cuts, low, high):
    gain = 1.0
    for dim, blocks in cuts:
        draws = jax.random.uniform(jax.random.fold_in(jax.random.fold_in(own_key, 6), dim), (blocks,), jnp.float32, low / len(cuts), high / len(cuts))
        gain = gain * jnp.repeat(jnp.exp(draws), extent[dim] // blocks).reshape((-1,) + (1,) * (len(extent) - 1 - dim))
    return gain


def gaussian_with(key, shape, scale, limit, cuts, heavy, held_as=jnp.bfloat16):
    array = scale * jax.random.normal(key, shape, jnp.float32)
    if cuts:
        array = array * level_of(key, shape, cuts, -0.22, 0.18)
    return jnp.clip(with_spikes(array, jax.random.fold_in(key, 3), *heavy), -limit, limit).astype(held_as)


def setup_inputs(seed: int = 0) -> dict:
    key_list = jax.random.split(jax.random.key(seed), 6)
    data = draw_data(jax.random.fold_in(key_list[5], 71), 0)
    rotations = gaussian_with(key_list[1], (ROT, TRIALS), TRIALS ** -0.5, 0.046875, ((0, 8), (1, 16)), (1, 0, 16, 2.0))
    span_order = jax.random.permutation(key_list[2], SPANS).astype(jnp.int32)
    adjacency = draw_adjacency(jax.random.fold_in(key_list[5], 71), 0)
    kernel = jnp.clip(jnp.exp(jax.random.uniform(key_list[4], (KERN,), jnp.float32, math.log(0.1), math.log(1.0))), 0.1, 1.0)
    return {"data": data, "rotations": rotations, "span_order": span_order, "adjacency": adjacency, "kernel": kernel}


def reference(data, rotations, span_order, adjacency, kernel):
    ordered = jnp.take(rotations.reshape(SPANS, SPAN, TRIALS), span_order, axis=0).reshape(ROT, TRIALS)
    flat = data.reshape(TRIALS, TIMES * SENS)
    sums = jnp.dot(ordered, flat, preferred_element_type=jnp.float32)
    power = lax.optimization_barrier(jnp.sum(jnp.square(flat.astype(jnp.float32)), axis=0)) / TRIALS
    score = sums / jnp.sqrt(power + 1e-05)[None, :]
    squared = (score * score).reshape(ROT * TIMES, SENS)
    links = adjacency.astype(jnp.float32)
    degree = lax.optimization_barrier(jnp.sum(links, axis=1))
    mix = (jnp.eye(SENS, dtype=jnp.float32) + links) / (1.0 + degree)[:, None]
    spread = jnp.dot(squared, mix.T, precision=lax.Precision.HIGHEST).reshape(ROT, TIMES, SENS)
    half = KERN // 2
    padded = jnp.pad(spread, ((0, 0), (half, half), (0, 0)))
    enhanced = jnp.zeros((ROT, TIMES, SENS), jnp.float32)
    for step in range(KERN):
        enhanced = enhanced + kernel[step] * padded[:, step:step + TIMES, :]
    return enhanced
```

```python
import functools

import jax
import jax.numpy as jnp
from jax import lax
from jax.experimental import pallas as pl
from jax.experimental.pallas import tpu as pltpu
from jax.sharding import Mesh
from jax.sharding import PartitionSpec as P

TRIAL = ("y", "xh", "c")
FEAT = ("xl", "z")
MESH = pl.DeviceIdType.MESH
F32, BF16, I16 = jnp.float32, jnp.bfloat16, jnp.int16
TOP = 32000.0

TRIALS, TDEV, SENS = 2048, 32, 128
BLOCK, BATCH, OWNED = 96, 384, 48
CHUNK, SLOTS = 128, 4
UNITS = BLOCK // 16
AWAY = ((0, 0), (1, 0), (0, 3), (0, 1), (0, 2), (1, 3), (1, 1), (1, 2))


def encode(v, q_at, s_at):
    top = jnp.maximum(jnp.max(jnp.abs(v), axis=0, keepdims=True), 1e-30)
    q_at(jnp.round(v * (TOP / top)).astype(jnp.int32).astype(I16))
    s_at(top * (1.0 / TOP))


def decode(q, s):
    return q.astype(jnp.int32).astype(F32) * s


def kernel(
    order, taps, data, rot, adj, out,
    raw, dv, rotg, lp, pw, part, part_in, acc,
    s1, s1s, r1, r1s, s2, s2s, r2, r2s, sx, sxs, rx, rxs, fin, place,
    a2s, a2ss, a2r, a2rs, hr, hrs, spread, turn,
    raw_sem, ag_s, ag_r, pw_s, pw_r, d_s, d_r, r1_s, r1_r, r2_s, r2_r, x_s, x_r, a_s, a_r, h_s, h_r,
):
    y, xh, c = lax.axis_index("y"), lax.axis_index("xh"), lax.axis_index("c")
    xl, z = lax.axis_index("xl"), lax.axis_index("z")
    me = y * 4 + xh * 2 + c
    f = xl * 4 + z
    pair = 8 * c + 2 * y + xh

    def dev(y_=y, xh_=xh, c_=c, xl_=xl, z_=z):
        return {"y": y_, "xh": xh_, "c": c_, "xl": xl_, "z": z_}

    def trial_dev(t):
        return dev(y_=t // 4, xh_=lax.rem(t // 2, 2), c_=lax.rem(t, 2))

    def feat_dev(g):
        return dev(xl_=g // 4, z_=lax.rem(g, 4))

    def plus(v, k, n):
        return lax.rem(v + k, n)

    def remote(src, dst, ss, rs, where):
        return pltpu.make_async_remote_copy(
            src_ref=src, dst_ref=dst, send_sem=ss, recv_sem=rs, device_id=where, device_id_type=MESH
        )

    z_up, z_dn = dev(z_=plus(z, 1, 4)), dev(z_=plus(z, 3, 4))
    y_up, y_dn = dev(y_=plus(y, 1, 4)), dev(y_=plus(y, 3, 4))
    across, mate, far = dev(xl_=1 - xl), dev(c_=1 - c), dev(xh_=1 - xh)
    f_up, f_dn = feat_dev(plus(f, 1, 8)), feat_dev(plus(f, 7, 8))

    chunks = TRIALS // CHUNK

    def load(i):
        k = lax.rem(i, SLOTS)
        return pltpu.make_async_copy(data.at[pl.ds(i * CHUNK, CHUNK)], raw.at[k], raw_sem.at[k])

    for i in range(SLOTS - 1):
        load(i).start()

    barrier = pltpu.get_barrier_semaphore()
    for where in (z_up, z_dn, across, f_up, f_dn):
        pl.semaphore_signal(barrier, inc=1, device_id=where, device_id_type=MESH)

    def greet(o, carry):
        pl.semaphore_signal(barrier, inc=1, device_id=trial_dev(plus(me, o, 16)), device_id_type=MESH)
        return carry

    lax.fori_loop(1, 16, greet, 0)
    pl.semaphore_wait(barrier, 20)

    lo, hi = pl.ds(0, BLOCK // 2), pl.ds(BLOCK // 2, BLOCK // 2)
    hops = [
        remote(rot, rotg.at[2], ag_s.at[0], ag_r.at[0], z_up),
        remote(rot, rotg.at[3], ag_s.at[1], ag_r.at[1], z_dn),
        remote(rot, rotg.at[1], ag_s.at[2], ag_r.at[2], across),
        remote(rotg.at[2, lo], rotg.at[4, lo], ag_s.at[3], ag_r.at[3], z_up),
        remote(rotg.at[3, hi], rotg.at[4, hi], ag_s.at[4], ag_r.at[4], z_dn),
        remote(rotg.at[1], rotg.at[5], ag_s.at[5], ag_r.at[5], z_up),
        remote(rotg.at[1], rotg.at[6], ag_s.at[6], ag_r.at[6], z_dn),
        remote(rotg.at[4, lo], rotg.at[7, lo], ag_s.at[7], ag_r.at[7], across),
        remote(rotg.at[4, hi], rotg.at[7, hi], ag_s.at[8], ag_r.at[8], across),
    ]
    for i in range(3):
        hops[i].start()

    def turn_in(i, total):
        @pl.when(i + SLOTS - 1 < chunks)
        def _():
            load(i + SLOTS - 1).start()

        load(i).wait()
        k = lax.rem(i, SLOTS)
        block = raw[k]
        wide = block.astype(F32)
        total = total + jnp.sum(wide * wide, axis=0)
        turned = jnp.swapaxes(block, 0, 1)
        rows = pl.ds(pl.multiple_of(i * CHUNK, CHUNK), CHUNK)
        for t in range(TDEV):
            dv[t // 2, rows, (t % 2) * SENS : (t % 2 + 1) * SENS] = turned[t]
        return total

    total = lax.fori_loop(0, chunks, turn_in, jnp.zeros((TDEV, SENS), F32))
    for p in range(TDEV // 2):
        lp[p] = total[2 * p : 2 * p + 2]

    def power_copy(o):
        t = plus(me, o, 16)
        theirs = 8 * lax.rem(t, 2) + t // 2
        return remote(lp.at[theirs], pw.at[o], pw_s.at[o], pw_r.at[o], trial_dev(t))

    def power_start(o, carry):
        power_copy(o).start()
        return carry

    lax.fori_loop(1, 16, power_start, 0)
    pw[0] = lp[pair]
    for slot, (dx, dz) in enumerate(AWAY):
        block = lax.rem(xl + dx, 2) * 4 + lax.rem(z + dz, 4)
        for w in range(UNITS):
            place[block * UNITS + w] = slot * UNITS + w
    rotg[0] = rot[...]

    def mate_copy(b, i):
        return remote(part.at[b, i], part_in.at[b, i], d_s.at[b, i], d_r.at[b, i], mate)

    def multiply(b, first, last):
        def body(i, carry):
            theirs = plus(y, lax.rem(3 * (i // 2) + 2, 4), 4) * 2 + lax.rem(i, 2)
            for half in (1 - c, c):
                left = rotg[4 * b : 4 * b + 4].reshape(BATCH, TRIALS)
                sums = jnp.dot(left, dv[8 * half + theirs], preferred_element_type=F32)
                if half is c:
                    acc[b, i] = sums
                else:
                    part[b, i] = sums
                    mate_copy(b, i).start()
            return carry

        lax.fori_loop(first, last, body, 0)

    def relay_copies(b, side, h):
        where = (y_up, y_dn)[side]
        return (
            remote(s1.at[b, side, h], r1.at[b, side, h], r1_s.at[b, side, h, 0], r1_r.at[b, side, h, 0], where),
            remote(s1s.at[b, side, h], r1s.at[b, side, h], r1_s.at[b, side, h, 1], r1_r.at[b, side, h, 1], where),
        )

    def owner_copies(b, side, h):
        where = (y_up, y_dn)[side]
        return (
            remote(s2.at[b, side, h], r2.at[b, side, h], r2_s.at[b, side, h, 0], r2_r.at[b, side, h, 0], where),
            remote(s2s.at[b, side, h], r2s.at[b, side, h], r2_s.at[b, side, h, 1], r2_r.at[b, side, h, 1], where),
        )

    def far_copies(b):
        return (
            remote(sx.at[b], rx.at[b], x_s.at[b, 0], x_r.at[b, 0], far),
            remote(sxs.at[b], rxs.at[b], x_s.at[b, 1], x_r.at[b, 1], far),
        )

    def start(copies):
        for copy in copies:
            copy.start()

    def arrive(copies):
        for copy in copies:
            copy.wait_recv()

    def rows_of(k):
        return pl.ds(k * BLOCK, BLOCK)

    def units_of(b, k):
        return pl.ds((4 * b + k) * UNITS, UNITS)

    def chip_sum(b, i, k):
        return acc[b, i, rows_of(k)] + part_in[b, i, rows_of(k)]

    def relay(b):
        for h in range(2):
            mate_copy(b, h).wait_recv()
            for side in range(2):
                for k in range(2):
                    encode(
                        chip_sum(b, h, 2 * side + k),
                        functools.partial(s1.__setitem__, (b, side, h, rows_of(k))),
                        functools.partial(s1s.__setitem__, (b, side, h, k)),
                    )
                start(relay_copies(b, side, h))

    def to_owner(b, side):
        for h in range(2):
            i = (2, 6)[side] + h
            mate_copy(b, i).wait_recv()
            arrive(relay_copies(b, side, h))
            for k in range(4):
                v = chip_sum(b, i, k)
                if k // 2 == side:
                    v = v + decode(r1[b, side, h, rows_of(k % 2)], r1s[b, side, h, k % 2])
                encode(
                    v,
                    functools.partial(s2.__setitem__, (b, side, h, rows_of(k))),
                    functools.partial(s2s.__setitem__, (b, side, h, k)),
                )
            start(owner_copies(b, side, h))

    def own(b, i, h, k):
        v = chip_sum(b, i, k)
        for side in range(2):
            v = v + decode(r2[b, side, h, rows_of(k)], r2s[b, side, h, k])
        return v

    def to_far(b):
        for h in range(2):
            mate_copy(b, 4 + h).wait_recv()
            for side in range(2):
                arrive(owner_copies(b, side, h))
        for k in range(4):
            encode(
                own(b, 5 - xh, 1 - xh, k),
                functools.partial(sx.__setitem__, (b, rows_of(k))),
                functools.partial(sxs.__setitem__, (b, k)),
            )
        start(far_copies(b))
        for k in range(4):
            fin[units_of(b, k)] = own(b, 4 + xh, xh, k).reshape(UNITS, 16, 2 * SENS)

    def finish(b):
        arrive(far_copies(b))
        for k in range(4):
            at = units_of(b, k)
            fin[at] = fin[at] + decode(rx[b, rows_of(k)], rxs[b, k]).reshape(UNITS, 16, 2 * SENS)

    for i in range(3):
        hops[i].wait_recv()
    for i in range(3, 7):
        hops[i].start()
    multiply(0, 0, 4)
    relay(0)
    for i in (3, 4):
        hops[i].wait_recv()
        hops[i + 4].start()
    multiply(0, 4, 8)
    to_owner(0, 0)
    to_owner(0, 1)
    for i in range(5, 9):
        hops[i].wait_recv()
    multiply(1, 0, 4)
    relay(1)
    to_far(0)
    multiply(1, 4, 8)
    to_owner(1, 0)
    to_owner(1, 1)
    finish(0)
    to_far(1)

    def power_wait(o, carry):
        power_copy(o).wait_recv()
        return carry

    lax.fori_loop(1, 16, power_wait, 0)
    power = jnp.sum(pw[...], axis=0) * (1.0 / (TRIALS * 16))
    scale = 1.0 / jnp.sqrt(power + 1e-05)
    scale = jnp.concatenate([scale[0:1], scale[1:2]], axis=1)
    finish(1)

    def unit_of(u):
        return place[8 * order[u // 8] + lax.rem(u, 8)]

    mine = pl.ds(2 * pair, 2)

    def score_copies(o):
        where = trial_dev(plus(me, o, 16))
        return (
            remote(a2s.at[o], a2r.at[mine], a_s.at[o, 0], a_r.at[o, 0], where),
            remote(a2ss.at[o], a2rs.at[mine], a_s.at[o, 1], a_r.at[o, 1], where),
        )

    def pick(o):
        t = plus(me, o, 16)
        v = jnp.concatenate([fin[unit_of(3 * t + j)] for j in range(3)], axis=0) * scale

        def put(to, q):
            to[0] = q[:, :SENS]
            to[1] = q[:, SENS:]

        return v, put

    def score_start(o, carry):
        v, put = pick(o)
        encode(v, functools.partial(put, a2s.at[o]), functools.partial(put, a2ss.at[o]))
        start(score_copies(o))
        return carry

    lax.fori_loop(1, 16, score_start, 0)
    v, put = pick(0)
    encode(v, functools.partial(put, a2r.at[mine]), functools.partial(put, a2rs.at[mine]))

    links = adj[...].astype(F32)
    at = (lax.broadcasted_iota(jnp.int32, (SENS, SENS), 0), lax.broadcasted_iota(jnp.int32, (SENS, SENS), 1))
    joined = (links + jnp.where(at[0] == at[1], 1.0, 0.0)).astype(BF16)
    contract = (((1,), (1,)), ((), ()))
    degree = lax.dot_general(jnp.ones((8, SENS), BF16), joined, contract, preferred_element_type=F32)
    share = 1.0 / degree[0:1]

    def score_wait(o, carry):
        arrive(score_copies(o))
        return carry

    lax.fori_loop(1, 16, score_wait, 0)
    edge = [
        remote(a2r.at[pl.ds(TDEV - 4, 4)], hr.at[0], h_s.at[0], h_r.at[0], f_up),
        remote(a2rs.at[pl.ds(TDEV - 4, 4)], hrs.at[0], h_s.at[1], h_r.at[1], f_up),
        remote(a2r.at[pl.ds(0, 4)], hr.at[1], h_s.at[2], h_r.at[2], f_dn),
        remote(a2rs.at[pl.ds(0, 4)], hrs.at[1], h_s.at[3], h_r.at[3], f_dn),
    ]
    start(edge)

    def mixed(q, s):
        v = decode(q, s)
        square = (v * v).reshape(4 * OWNED, SENS)
        head = square.astype(BF16)
        rest = (square - head.astype(F32)).astype(BF16)
        both = lax.dot_general(head, joined, contract, preferred_element_type=F32) + lax.dot_general(
            rest, joined, contract, preferred_element_type=F32
        )
        return (both * share).reshape(4, OWNED, SENS)

    def mix_step(i, carry):
        four = pl.ds(4 * i, 4)
        spread[pl.ds(4 * i + 4, 4)] = mixed(a2r[four], a2rs[four])
        return carry

    lax.fori_loop(0, TDEV // 4, mix_step, 0)
    arrive(edge)
    spread[0:4] = jnp.where(f > 0, mixed(hr[0], hrs[0]), 0.0)
    spread[TDEV + 4 : TDEV + 8] = jnp.where(f < 7, mixed(hr[1], hrs[1]), 0.0)

    def smooth(i, carry):
        for j in range(8):
            line = jnp.zeros((OWNED, SENS), F32)
            for k in range(9):
                line = line + taps[k] * spread[8 * i + j + k]
            turn[j] = line
        out[:, pl.ds(pl.multiple_of(8 * i, 8), 8), :] = jnp.swapaxes(turn[...], 0, 1)
        return carry

    lax.fori_loop(0, TDEV // 8, smooth, 0)

    for hop in hops:
        hop.wait_send()

    def gone(o, carry):
        power_copy(o).wait_send()
        for copy in score_copies(o):
            copy.wait_send()
        return carry

    lax.fori_loop(1, 16, gone, 0)
    for b in range(2):
        for i in range(8):
            mate_copy(b, i).wait_send()
        for side in range(2):
            for h in range(2):
                for copy in relay_copies(b, side, h) + owner_copies(b, side, h):
                    copy.wait_send()
        for copy in far_copies(b):
            copy.wait_send()
    for copy in edge:
        copy.wait_send()


def per_device(data, rotations, span_order, adjacency, taps):
    vmem, smem, dma = pltpu.VMEM, pltpu.SMEM, pltpu.SemaphoreType.DMA
    spec = lambda space: pl.BlockSpec(memory_space=space)
    wide = 2 * SENS
    scratch = [
        vmem((SLOTS, CHUNK, TDEV, SENS), BF16),
        vmem((TDEV // 2, TRIALS, wide), BF16),
        vmem((8, BLOCK, TRIALS), BF16),
        vmem((16, 2, SENS), F32),
        vmem((16, 2, SENS), F32),
        vmem((2, 8, BATCH, wide), F32),
        vmem((2, 8, BATCH, wide), F32),
        vmem((2, 8, BATCH, wide), F32),
        vmem((2, 2, 2, BATCH // 2, wide), I16),
        vmem((2, 2, 2, 2, 1, wide), F32),
        vmem((2, 2, 2, BATCH // 2, wide), I16),
        vmem((2, 2, 2, 2, 1, wide), F32),
        vmem((2, 2, 2, BATCH, wide), I16),
        vmem((2, 2, 2, 4, 1, wide), F32),
        vmem((2, 2, 2, BATCH, wide), I16),
        vmem((2, 2, 2, 4, 1, wide), F32),
        vmem((2, BATCH, wide), I16),
        vmem((2, 4, 1, wide), F32),
        vmem((2, BATCH, wide), I16),
        vmem((2, 4, 1, wide), F32),
        vmem((8 * UNITS, 16, wide), F32),
        smem((8 * UNITS,), jnp.int32),
        vmem((16, 2, OWNED, SENS), I16),
        vmem((16, 2, 1, SENS), F32),
        vmem((TDEV, OWNED, SENS), I16),
        vmem((TDEV, 1, SENS), F32),
        vmem((2, 4, OWNED, SENS), I16),
        vmem((2, 4, 1, SENS), F32),
        vmem((TDEV + 8, OWNED, SENS), F32),
        vmem((8, OWNED, SENS), F32),
        dma((SLOTS,)),
        dma((9,)), dma((9,)),
        dma((16,)), dma((16,)),
        dma((2, 8)), dma((2, 8)),
        dma((2, 2, 2, 2)), dma((2, 2, 2, 2)),
        dma((2, 2, 2, 2)), dma((2, 2, 2, 2)),
        dma((2, 2)), dma((2, 2)),
        dma((16, 2)), dma((16, 2)),
        dma((4,)), dma((4,)),
    ]
    return pl.pallas_call(
        kernel,
        out_shape=jax.ShapeDtypeStruct((OWNED, TDEV, SENS), F32),
        in_specs=[spec(smem), spec(smem), spec(pl.ANY), spec(vmem), spec(vmem)],
        out_specs=spec(vmem),
        scratch_shapes=scratch,
        compiler_params=pltpu.CompilerParams(
            collective_id=0, has_side_effects=True, vmem_limit_bytes=66000000
        ),
    )(span_order, taps, data, rotations, adjacency)


def solution(mesh):
    torus = Mesh(mesh.devices.reshape(4, 2, 2, 2, 4), TRIAL + FEAT)
    in_specs = (P(TRIAL, FEAT, None), P(FEAT, TRIAL), P(), P(), P())
    return jax.shard_map(
        per_device, mesh=torus, in_specs=in_specs, out_specs=P(TRIAL, FEAT, None), check_vma=False
    )
```
